32 devices in a mesh: row: 8 (over y, x, core), col: 4 (over z).
Axes of the slice: x: 2, y: 2, z: 4, core: 2. Of those that a mesh axis runs over, the one named last changes fastest.
Arguments:
- species: float32 [4, 64, 32, 256], P(None, None, 'row', 'col'), may hold values from -6 to 6
- symbol_x: float32 [64], replicated, may hold values from 0.3 to 3
- symbol_y: float32 [32], replicated, may hold values from 0.3 to 3
- symbol_z: float32 [256], replicated, may hold values from 0.3 to 3
Outputs:
- coefficients: float32 [4, 64, 32, 256], P(None, 'row', 'col')
The draws below stay inside these ranges and needn't reach their ends.
All inputs are finite; a program needn't handle non-finite values.
Results may differ from the reference program's by a relative error of at most 0.00007.
Values sent between devices are 32-bit elements; how exact they have to be, the bound alone decides.
A program may use at most 64 MiB of HBM per device.

```python
import jax
import jax.numpy as jnp
from jax import lax

GRID_X = 64
GRID_Y = 32
GRID_Z = 256
FIELDS = 4


def levels(key, extent, split, smallest, largest):
    def one(axis_at, parts):
        draws = jax.random.uniform(jax.random.fold_in(jax.random.fold_in(key, 6), axis_at), (parts,), jnp.float32, smallest / len(split), largest / len(split))
        return jnp.repeat(jnp.exp(draws), extent[axis_at] // parts).reshape((-1,) + (1,) * (len(extent) - axis_at - 1))

    factor_of = one(*split[0])
    for cut in split[1:]:
        factor_of = factor_of * one(*cut)
    return factor_of


def bell_draw(key, shape, width, bound, pieces=(), kind=jnp.bfloat16):
    array = width * jax.random.normal(key, shape, jnp.float32)
    if pieces:
        array = array * levels(key, shape, pieces, -0.22, 0.18)
    return jnp.clip(array, -bound, bound).astype(kind)


def setup_inputs(seed: int = 0) -> dict:
    key_of = jax.random.split(jax.random.key(seed), 5)
    species = bell_draw(key_of[0], (FIELDS, GRID_X, GRID_Y, GRID_Z), 1.0, 6.0, ((2, 8), (3, 4)), jnp.float32)
    symbol_x = jnp.clip(jax.random.uniform(key_of[1], (GRID_X,), jnp.float32, 0.3, 3.0), 0.3, 3.0)
    symbol_y = jnp.clip(jax.random.uniform(key_of[2], (GRID_Y,), jnp.float32, 0.3, 3.0), 0.3, 3.0)
    symbol_z = jnp.clip(jax.random.uniform(key_of[3], (GRID_Z,), jnp.float32, 0.3, 3.0), 0.3, 3.0)
    return dict(species=species, symbol_x=symbol_x, symbol_y=symbol_y, symbol_z=symbol_z)


def transform_table(count):
    rank = jnp.arange(count)
    angle = (jnp.pi / (count + 1)) * (((rank[:, None] + 1) * (rank[None, :] + 1)) % (2 * count + 2)).astype(jnp.float32)
    return jnp.sin(angle) * (2.0 / (count + 1)) ** 0.5


def transform_dim(values, dim):
    moved = jnp.tensordot(values, transform_table(values.shape[dim]), axes=([dim], [0]), precision=lax.Precision.HIGHEST)
    return jnp.moveaxis(moved, -1, dim)


def reference(species, symbol_x, symbol_y, symbol_z):
    coefficients = species
    coefficients = transform_dim(coefficients, 1)
    coefficients = transform_dim(coefficients, 2)
    coefficients = transform_dim(coefficients, 3)
    symbol = symbol_x[:, None, None] + symbol_y[None, :, None] + symbol_z[None, None, :]
    coefficients = coefficients / symbol
    return coefficients
```

```python
import functools

import jax
import jax.numpy as jnp
import ml_dtypes
import numpy as np
from jax import lax
from jax.experimental import pallas as pl
from jax.experimental.pallas import tpu as pltpu
from jax.sharding import PartitionSpec as P

MESH = pl.DeviceIdType.MESH
LANES = 128


def table(count):
    rank = np.arange(count, dtype=np.int64) + 1
    angle = np.pi / (count + 1) * ((rank[:, None] * rank[None, :]) % (2 * count + 2))
    return (np.sin(angle) * (2.0 / (count + 1)) ** 0.5).astype(np.float32)


def halves(values):
    high = values.astype(ml_dtypes.bfloat16)
    low = (values - high.astype(np.float32)).astype(ml_dtypes.bfloat16)
    return np.stack([high, low])


def split(values):
    high = values.astype(jnp.bfloat16)
    low = (values - high.astype(jnp.float32)).astype(jnp.bfloat16)
    return high, low


def dot(a, b):
    return jnp.dot(a, b, preferred_element_type=jnp.float32)


def left_dot(high, low, data):
    data_high, data_low = data
    return dot(high, data_high) + dot(high, data_low) + dot(low, data_high)


def partner(me, step, count):
    if count & (count - 1):
        return lax.rem(me + step, count)
    to, bit = me, 1
    while bit < count:
        if step & bit:
            to = to + bit * (1 - 2 * lax.rem(me // bit, 2))
        bit *= 2
    return to


def kernel(
    dims,
    species, symbol_x, symbol_y, symbol_z, table_x, table_y, table_z,
    out,
    space, mx, my, mz, sx, sy, sz, send_a, recv_a, send_b, recv_b, inverse,
    load_sem, a_send, a_recv, b_send, b_recv,
):
    fields, pack, rows, cols, cuts, xc, yb, zl = dims
    groups = fields // pack
    row, col = lax.axis_index("row"), lax.axis_index("col")

    loads = [
        pltpu.make_async_copy(src, dst, load_sem.at[i])
        for i, (src, dst) in enumerate([
            (species, space), (table_x, mx), (symbol_x, sx), (symbol_y, sy), (symbol_z, sz), (table_y, my), (table_z, mz),
        ])
    ]
    for load in loads:
        load.start()
    row_steps = list(range(rows - 1, 0, -1))
    col_steps = list(range(cols - 1, 0, -1))
    barrier = pltpu.get_barrier_semaphore()
    for step in col_steps:
        pl.semaphore_signal(barrier, inc=1, device_id={"col": partner(col, step, cols)}, device_id_type=MESH)
    for step in row_steps:
        pl.semaphore_signal(barrier, inc=1, device_id={"row": partner(row, step, rows)}, device_id_type=MESH)

    loads[0].wait()
    data = []
    for g in range(groups):
        packed = jnp.concatenate([space[g * pack + i] for i in range(pack)], axis=-1)
        data.append(split(packed))
    loads[1].wait()

    chunks = [(q, g) for q in range(cuts) for g in range(groups)]
    for i, (q, g) in enumerate(chunks):
        send_a[q, g] = left_dot(mx[0, q], mx[1, q], data[g]).reshape(send_a.shape[2:])
        if i == 0:
            pl.semaphore_wait(barrier, len(row_steps) + len(col_steps))
        for step in row_steps:
            to = partner(row, step, rows)
            pltpu.make_async_remote_copy(
                src_ref=send_a.at[q, g, to], dst_ref=recv_a.at[q, g, row],
                send_sem=a_send.at[i, step], recv_sem=a_recv.at[i, step],
                device_id={"row": to}, device_id_type=MESH,
            ).start()
        recv_a[q, g, row] = send_a[q, g, row]

    for load in loads[2:]:
        load.wait()
    part_y = jnp.zeros((yb, 1), jnp.float32)
    at = lax.broadcasted_iota(jnp.int32, (yb, 1), 0)
    for j in range(yb):
        part_y = jnp.where(at == j, sy[col * yb + j], part_y)
    for i in range(cuts * xc):
        inverse[i] = 1.0 / ((sx[row * (cuts * xc) + i] + part_y) + sz[...])

    for i, (q, g) in enumerate(chunks):
        for step in row_steps:
            to = partner(row, step, rows)
            pltpu.make_async_remote_copy(
                src_ref=send_a.at[q, g, to], dst_ref=recv_a.at[q, g, row],
                send_sem=a_send.at[i, step], recv_sem=a_recv.at[i, step],
                device_id={"row": to}, device_id_type=MESH,
            ).wait_recv()
        lines = recv_a[q, g].reshape(-1, LANES)
        send_b[q, g] = left_dot(my[0], my[1], split(lines)).reshape(send_b.shape[2:])
        for step in col_steps:
            to = partner(col, step, cols)
            pltpu.make_async_remote_copy(
                src_ref=send_b.at[q, g, to], dst_ref=recv_b.at[q, g, col],
                send_sem=b_send.at[i, step], recv_sem=b_recv.at[i, step],
                device_id={"col": to}, device_id_type=MESH,
            ).start()
        recv_b[q, g, col] = send_b[q, g, col]

    for i, (q, g) in enumerate(chunks):
        for step in col_steps:
            to = partner(col, step, cols)
            pltpu.make_async_remote_copy(
                src_ref=send_b.at[q, g, to], dst_ref=recv_b.at[q, g, col],
                send_sem=b_send.at[i, step], recv_sem=b_recv.at[i, step],
                device_id={"col": to}, device_id_type=MESH,
            ).wait_recv()
        blocks = [recv_b[q, g, c] for c in range(cols)]
        lines = jnp.concatenate(
            [jnp.concatenate([b[:, k * zl:(k + 1) * zl] for b in blocks], axis=-1) for k in range(pack)], axis=0
        )
        high, low = split(lines)
        result = dot(high, mz[0]) + dot(high, mz[1]) + dot(low, mz[0])
        factor = inverse[q * xc:(q + 1) * xc].reshape(xc * yb, -1)
        for k in range(pack):
            out[g * pack + k, q * xc * yb:(q + 1) * xc * yb] = result[k * xc * yb:(k + 1) * xc * yb] * factor

    for i, (q, g) in enumerate(chunks):
        for step in row_steps:
            to = partner(row, step, rows)
            pltpu.make_async_remote_copy(
                src_ref=send_a.at[q, g, to], dst_ref=recv_a.at[q, g, row],
                send_sem=a_send.at[i, step], recv_sem=a_recv.at[i, step],
                device_id={"row": to}, device_id_type=MESH,
            ).wait_send()
        for step in col_steps:
            to = partner(col, step, cols)
            pltpu.make_async_remote_copy(
                src_ref=send_b.at[q, g, to], dst_ref=recv_b.at[q, g, col],
                send_sem=b_send.at[i, step], recv_sem=b_recv.at[i, step],
                device_id={"col": to}, device_id_type=MESH,
            ).wait_send()


def on_device(rows, cols, species, symbol_x, symbol_y, symbol_z):
    fields, x, yl, zl = species.shape
    y, z = symbol_y.shape[0], symbol_z.shape[0]
    xb, yb = x // rows, y // cols
    pack = LANES // zl
    groups = fields // pack
    cuts = 2
    xc = xb // cuts

    hx = table(x)
    eye = np.eye(yl, dtype=np.float32)
    full_x = np.einsum("rqia,yb->qriyab", hx.T.reshape(rows, cuts, xc, x), eye).reshape(cuts, rows * xc * yl, x * yl)
    hy = table(y).T.reshape(cols, yb, rows, yl)
    full_y = np.einsum("cmry,ij->cimrjy", hy, np.eye(xc, dtype=np.float32)).reshape(cols * xc * yb, rows * xc * yl)
    tables = [halves(full_x), halves(full_y), halves(table(z))]

    any_space = pl.BlockSpec(memory_space=pltpu.MemorySpace.HBM)
    chunks = cuts * groups
    a_shape = (cuts, groups, rows, xc * yl, LANES)
    b_shape = (cuts, groups, cols, xc * yb, LANES)
    dma = pltpu.SemaphoreType.DMA
    out = pl.pallas_call(
        functools.partial(kernel, (fields, pack, rows, cols, cuts, xc, yb, zl)),
        out_shape=jax.ShapeDtypeStruct((fields, xb * yb, z), jnp.float32),
        in_specs=[any_space] * 7,
        out_specs=pl.BlockSpec(memory_space=pltpu.MemorySpace.VMEM),
        scratch_shapes=[
            pltpu.VMEM((fields, x * yl, zl), jnp.float32),
            pltpu.VMEM(tables[0].shape, jnp.bfloat16),
            pltpu.VMEM(tables[1].shape, jnp.bfloat16),
            pltpu.VMEM(tables[2].shape, jnp.bfloat16),
            pltpu.SMEM((x,), jnp.float32),
            pltpu.SMEM((y,), jnp.float32),
            pltpu.VMEM((1, z), jnp.float32),
            pltpu.VMEM(a_shape, jnp.float32),
            pltpu.VMEM(a_shape, jnp.float32),
            pltpu.VMEM(b_shape, jnp.float32),
            pltpu.VMEM(b_shape, jnp.float32),
            pltpu.VMEM((xb, yb, z), jnp.float32),
            dma((7,)),
            dma((chunks, rows)),
            dma((chunks, rows)),
            dma((chunks, cols)),
            dma((chunks, cols)),
        ],
        compiler_params=pltpu.CompilerParams(
            collective_id=0, has_side_effects=True, vmem_limit_bytes=60 * 1024 * 1024
        ),
    )(
        species.reshape(fields, x * yl, zl), symbol_x, symbol_y, symbol_z.reshape(1, z),
        *[jnp.asarray(t) for t in tables],
    )
    return out.reshape(fields, xb, yb, z)


def solution(mesh):
    placed = (P(None, None, "row", "col"), P(), P(), P())
    return jax.shard_map(
        functools.partial(on_device, mesh.shape["row"], mesh.shape["col"]),
        mesh=mesh,
        in_specs=placed,
        out_specs=P(None, "row", "col", None),
        check_vma=False,
    )
```

```python
import functools

import jax
import jax.numpy as jnp
import ml_dtypes
import numpy as np
from jax import lax
from jax.experimental import pallas as pl
from jax.experimental.pallas import tpu as pltpu
from jax.sharding import PartitionSpec as P

MESH = pl.DeviceIdType.MESH
LANES = 128


def table(count):
    rank = np.arange(count, dtype=np.int64) + 1
    angle = np.pi / (count + 1) * ((rank[:, None] * rank[None, :]) % (2 * count + 2))
    return (np.sin(angle) * (2.0 / (count + 1)) ** 0.5).astype(np.float32)


def halves(values):
    high = values.astype(ml_dtypes.bfloat16)
    low = (values - high.astype(np.float32)).astype(ml_dtypes.bfloat16)
    return np.stack([high, low])


def split(values):
    high = values.astype(jnp.bfloat16)
    low = (values - high.astype(jnp.float32)).astype(jnp.bfloat16)
    return high, low


def side_by_side(values):
    return jnp.concatenate(split(values), axis=-1)


def dot(a, b):
    return jnp.dot(a, b, preferred_element_type=jnp.float32)


def left_dot(both, data):
    count, width = both.shape[0] // 2, data.shape[-1] // 2
    terms = dot(both, data)
    sides = terms[:, :width] + terms[:, width:]
    return sides[:count] + sides[count:]


def batches(count):
    return [[i] for i in range(count - 2)] + [[count - 2, count - 1]]


def partner(me, step, count):
    if count & (count - 1):
        return lax.rem(me + step, count)
    to, bit = me, 1
    while bit < count:
        if step & bit:
            to = to + bit * (1 - 2 * lax.rem(me // bit, 2))
        bit *= 2
    return to


def kernel(
    dims,
    species, symbol_x, symbol_y, symbol_z, table_x, table_y, table_z,
    out,
    space, mx, my, mz, sx, sy, sz, send_a, recv_a, send_b, recv_b, inverse, held,
    load_sem, store_sem, a_send, a_recv, b_send, b_recv,
):
    fields, pack, rows, cols, cuts, xc, yb, zl = dims
    groups = fields // pack
    row, col = lax.axis_index("row"), lax.axis_index("col")

    pieces = [(species.at[f], space.at[f]) for f in range(fields)]
    pieces += [(table_x.at[q], mx.at[q]) for q in range(cuts)]
    pieces += [(symbol_x, sx), (symbol_y, sy), (symbol_z, sz), (table_y, my), (table_z, mz)]
    loads = [pltpu.make_async_copy(src, dst, load_sem.at[i]) for i, (src, dst) in enumerate(pieces)]
    urgent = list(range(pack)) + [fields]
    for i in urgent:
        loads[i].start()
    row_steps = list(range(rows - 1, 0, -1))
    col_steps = list(range(cols - 1, 0, -1))
    barrier = pltpu.get_barrier_semaphore()
    for step in col_steps:
        pl.semaphore_signal(barrier, inc=1, device_id={"col": partner(col, step, cols)}, device_id_type=MESH)
    for step in row_steps:
        pl.semaphore_signal(barrier, inc=1, device_id={"row": partner(row, step, rows)}, device_id_type=MESH)
    for i in range(fields + cuts):
        if i not in urgent:
            loads[i].start()

    chunks = [(q, g) for g in range(groups) for q in range(cuts)]
    for i, (q, g) in enumerate(chunks):
        if q == 0:
            for k in range(pack):
                loads[g * pack + k].wait()
            data = side_by_side(jnp.concatenate([space[g * pack + k] for k in range(pack)], axis=-1))
        if g == 0:
            loads[fields + q].wait()
        send_a[q, g] = left_dot(mx[q], data).reshape(send_a.shape[2:])
        if i == 0:
            for load in loads[fields + cuts:]:
                load.start()
            pl.semaphore_wait(barrier, len(row_steps) + len(col_steps))
        for step in row_steps:
            to = partner(row, step, rows)
            pltpu.make_async_remote_copy(
                src_ref=send_a.at[q, g, to], dst_ref=recv_a.at[q, g, row],
                send_sem=a_send, recv_sem=a_recv.at[i],
                device_id={"row": to}, device_id_type=MESH,
            ).start()
        recv_a[q, g, row] = send_a[q, g, row]

    for load in loads[fields + cuts:]:
        load.wait()
    part_y = jnp.zeros((yb, 1), jnp.float32)
    at = lax.broadcasted_iota(jnp.int32, (yb, 1), 0)
    for j in range(yb):
        part_y = jnp.where(at == j, sy[col * yb + j], part_y)
    for i in range(cuts * xc):
        inverse[i] = 1.0 / ((sx[row * (cuts * xc) + i] + part_y) + sz[...])

    for i, (q, g) in enumerate(chunks):
        arrived = recv_a.at[q, g, pl.ds(0, rows - 1)]
        pltpu.make_async_copy(arrived, arrived, a_recv.at[i]).wait()
        lines = recv_a[q, g].reshape(-1, LANES)
        send_b[q, g] = left_dot(my[...], side_by_side(lines)).reshape(send_b.shape[2:])
        for step in col_steps:
            to = partner(col, step, cols)
            pltpu.make_async_remote_copy(
                src_ref=send_b.at[q, g, to], dst_ref=recv_b.at[q, g, col],
                send_sem=b_send, recv_sem=b_recv.at[i],
                device_id={"col": to}, device_id_type=MESH,
            ).start()
        recv_b[q, g, col] = send_b[q, g, col]

    stores = []
    height = xc * yb
    for batch in batches(len(chunks)):
        lines = []
        for i in batch:
            q, g = chunks[i]
            arrived = recv_b.at[q, g, pl.ds(0, cols - 1)]
            pltpu.make_async_copy(arrived, arrived, b_recv.at[i]).wait()
            blocks = [recv_b[q, g, c] for c in range(cols)]
            for k in range(pack):
                lines.append(jnp.concatenate([b[:, k * zl:(k + 1) * zl] for b in blocks], axis=-1))
        high, low = split(jnp.concatenate(lines, axis=0))
        most = dot(jnp.concatenate([high, low], axis=0), mz[0])
        count = high.shape[0]
        result = most[:count] + most[count:] + dot(high, mz[1])
        for n, i in enumerate(batch):
            q, g = chunks[i]
            factor = inverse[q * xc:(q + 1) * xc].reshape(height, -1)
            for k in range(pack):
                at_line = (n * pack + k) * height
                held[i, k] = result[at_line:at_line + height] * factor
            stores.append(pltpu.make_async_copy(
                held.at[i], out.at[pl.ds(g * pack, pack), pl.ds(q * height, height)], store_sem.at[i]
            ))
            stores[-1].start()

    sent = send_a.at[:, :, pl.ds(0, rows - 1)]
    pltpu.make_async_copy(sent, sent, a_send).wait()
    sent = send_b.at[:, :, pl.ds(0, cols - 1)]
    pltpu.make_async_copy(sent, sent, b_send).wait()
    for store in stores:
        store.wait()


def on_device(rows, cols, species, symbol_x, symbol_y, symbol_z):
    fields, x, yl, zl = species.shape
    y, z = symbol_y.shape[0], symbol_z.shape[0]
    xb, yb = x // rows, y // cols
    pack = LANES // zl
    groups = fields // pack
    cuts = 2
    xc = xb // cuts

    hx = table(x)
    eye = np.eye(yl, dtype=np.float32)
    full_x = np.einsum("rqia,yb->qriyab", hx.T.reshape(rows, cuts, xc, x), eye).reshape(cuts, rows * xc * yl, x * yl)
    hy = table(y).T.reshape(cols, yb, rows, yl)
    full_y = np.einsum("cmry,ij->cimrjy", hy, np.eye(xc, dtype=np.float32)).reshape(cols * xc * yb, rows * xc * yl)
    tables = [
        np.concatenate(list(halves(full_x)), axis=1), np.concatenate(list(halves(full_y)), axis=0), halves(table(z))
    ]

    any_space = pl.BlockSpec(memory_space=pltpu.MemorySpace.HBM)
    chunks = cuts * groups
    a_shape = (cuts, groups, rows, xc * yl, LANES)
    b_shape = (cuts, groups, cols, xc * yb, LANES)
    dma = pltpu.SemaphoreType.DMA
    out = pl.pallas_call(
        functools.partial(kernel, (fields, pack, rows, cols, cuts, xc, yb, zl)),
        out_shape=pltpu.MemorySpace.VMEM((fields, xb * yb, z), jnp.float32),
        in_specs=[any_space] * 7,
        out_specs=pl.BlockSpec(memory_space=pl.ANY),
        scratch_shapes=[
            pltpu.VMEM((fields, x * yl, zl), jnp.float32),
            pltpu.VMEM(tables[0].shape, jnp.bfloat16),
            pltpu.VMEM(tables[1].shape, jnp.bfloat16),
            pltpu.VMEM(tables[2].shape, jnp.bfloat16),
            pltpu.SMEM((x,), jnp.float32),
            pltpu.SMEM((y,), jnp.float32),
            pltpu.VMEM((1, z), jnp.float32),
            pltpu.VMEM(a_shape, jnp.float32),
            pltpu.VMEM(a_shape, jnp.float32),
            pltpu.VMEM(b_shape, jnp.float32),
            pltpu.VMEM(b_shape, jnp.float32),
            pltpu.VMEM((xb, yb, z), jnp.float32),
            pltpu.VMEM((chunks, pack, xc * yb, z), jnp.float32),
            dma((fields + cuts + 5,)),
            dma((chunks,)),
            dma,
            dma((chunks,)),
            dma,
            dma((chunks,)),
        ],
        compiler_params=pltpu.CompilerParams(
            collective_id=0, has_side_effects=True, vmem_limit_bytes=60 * 1024 * 1024
        ),
    )(
        species.reshape(fields, x * yl, zl), symbol_x, symbol_y, symbol_z.reshape(1, z),
        *[jnp.asarray(t) for t in tables],
    )
    return out.reshape(fields, xb, yb, z)


def solution(mesh):
    placed = (P(None, None, "row", "col"), P(), P(), P())
    return jax.shard_map(
        functools.partial(on_device, mesh.shape["row"], mesh.shape["col"]),
        mesh=mesh,
        in_specs=placed,
        out_specs=P(None, "row", "col", None),
        check_vma=False,
    )
```

```python
import functools

import jax
import jax.numpy as jnp
import ml_dtypes
import numpy as np
from jax import lax
from jax.experimental import pallas as pl
from jax.experimental.pallas import tpu as pltpu
from jax.sharding import PartitionSpec as P

MESH = pl.DeviceIdType.MESH
LANES = 128


def table(count):
    rank = np.arange(count, dtype=np.int64) + 1
    angle = np.pi / (count + 1) * ((rank[:, None] * rank[None, :]) % (2 * count + 2))
    return (np.sin(angle) * (2.0 / (count + 1)) ** 0.5).astype(np.float32)


def halves(values):
    high = values.astype(ml_dtypes.bfloat16)
    low = (values - high.astype(np.float32)).astype(ml_dtypes.bfloat16)
    return np.stack([high, low])


def split(values):
    high = values.astype(jnp.bfloat16)
    low = (values - high.astype(jnp.float32)).astype(jnp.bfloat16)
    return high, low


def side_by_side(values):
    return jnp.concatenate(split(values), axis=-1)


def dot(a, b):
    return jnp.dot(a, b, preferred_element_type=jnp.float32)


def left_dot(both, data):
    count, width = both.shape[0] // 2, data.shape[-1] // 2
    terms = dot(both, data)
    sides = terms[:, :width] + terms[:, width:]
    return sides[:count] + sides[count:]


def far_first(me, slot, count):
    if count != 4:
        return partner(me, count - 1 - slot, count)
    inner = lax.rem((me + 1) // 2, 2)
    outer_to, inner_to = (partner(me, step, count) for step in ((3, 2), (2, 3), (1, 1))[slot])
    return outer_to + (inner_to - outer_to) * inner


def batches(count):
    return [[i] for i in range(count - 2)] + [[count - 2, count - 1]]


def partner(me, step, count):
    if count & (count - 1):
        return lax.rem(me + step, count)
    to, bit = me, 1
    while bit < count:
        if step & bit:
            to = to + bit * (1 - 2 * lax.rem(me // bit, 2))
        bit *= 2
    return to


def kernel(
    dims,
    species, symbol_x, symbol_y, symbol_z, table_x, table_y, table_z,
    out,
    space, mx, my, mz, sx, sy, sz, send_a, recv_a, send_b, recv_b, inverse, held,
    load_sem, store_sem, a_send, a_recv, b_send, b_recv,
):
    fields, pack, rows, cols, cuts, xc, yb, zl = dims
    groups = fields // pack
    row, col = lax.axis_index("row"), lax.axis_index("col")

    pieces = [(species.at[f], space.at[f]) for f in range(fields)]
    pieces += [(table_x.at[q], mx.at[q]) for q in range(cuts)]
    pieces += [(symbol_x, sx), (symbol_y, sy), (symbol_z, sz), (table_y, my), (table_z, mz)]
    loads = [pltpu.make_async_copy(src, dst, load_sem.at[i]) for i, (src, dst) in enumerate(pieces)]
    urgent = list(range(pack)) + [fields]
    for i in urgent:
        loads[i].start()
    row_steps = list(range(rows - 1, 0, -1))
    col_steps = list(range(cols - 1, 0, -1))
    barrier = pltpu.get_barrier_semaphore()
    for step in col_steps:
        pl.semaphore_signal(barrier, inc=1, device_id={"col": partner(col, step, cols)}, device_id_type=MESH)
    for step in row_steps:
        pl.semaphore_signal(barrier, inc=1, device_id={"row": partner(row, step, rows)}, device_id_type=MESH)
    for i in range(fields + cuts):
        if i not in urgent:
            loads[i].start()

    chunks = [(q, g) for g in range(groups) for q in range(cuts)]
    for i, (q, g) in enumerate(chunks):
        if q == 0:
            for k in range(pack):
                loads[g * pack + k].wait()
            data = side_by_side(jnp.concatenate([space[g * pack + k] for k in range(pack)], axis=-1))
        if g == 0:
            loads[fields + q].wait()
        send_a[q, g] = left_dot(mx[q], data).reshape(send_a.shape[2:])
        if i == 0:
            for load in loads[fields + cuts:]:
                load.start()
            pl.semaphore_wait(barrier, len(row_steps) + len(col_steps))
        for step in row_steps:
            to = partner(row, step, rows)
            pltpu.make_async_remote_copy(
                src_ref=send_a.at[q, g, to], dst_ref=recv_a.at[q, g, row],
                send_sem=a_send, recv_sem=a_recv.at[i],
                device_id={"row": to}, device_id_type=MESH,
            ).start()
        recv_a[q, g, row] = send_a[q, g, row]

    for load in loads[fields + cuts:]:
        load.wait()
    part_y = jnp.zeros((yb, 1), jnp.float32)
    at = lax.broadcasted_iota(jnp.int32, (yb, 1), 0)
    for j in range(yb):
        part_y = jnp.where(at == j, sy[col * yb + j], part_y)
    for i in range(cuts * xc):
        inverse[i] = 1.0 / ((sx[row * (cuts * xc) + i] + part_y) + sz[...])

    def pass_on(i, slot):
        q, g = chunks[i]
        to = far_first(col, slot, cols)
        pltpu.make_async_remote_copy(
            src_ref=send_b.at[q, g, to], dst_ref=recv_b.at[q, g, col],
            send_sem=b_send, recv_sem=b_recv.at[i],
            device_id={"col": to}, device_id_type=MESH,
        ).start()

    for i, (q, g) in enumerate(chunks):
        arrived = recv_a.at[q, g, pl.ds(0, rows - 1)]
        pltpu.make_async_copy(arrived, arrived, a_recv.at[i]).wait()
        lines = recv_a[q, g].reshape(-1, LANES)
        send_b[q, g] = left_dot(my[...], side_by_side(lines)).reshape(send_b.shape[2:])
        for slot in range(1):
            pass_on(i, slot)
        recv_b[q, g, col] = send_b[q, g, col]

    for i, slot in [(i, s) for s in range(1, cols - 1) for i in range(len(chunks)) ]:
        pass_on(i, slot)
    stores = []
    height = xc * yb
    for batch in batches(len(chunks)):
        lines = []
        for i in batch:
            q, g = chunks[i]
            arrived = recv_b.at[q, g, pl.ds(0, cols - 1)]
            pltpu.make_async_copy(arrived, arrived, b_recv.at[i]).wait()
            blocks = [recv_b[q, g, c] for c in range(cols)]
            for k in range(pack):
                lines.append(jnp.concatenate([b[:, k * zl:(k + 1) * zl] for b in blocks], axis=-1))
        high, low = split(jnp.concatenate(lines, axis=0))
        most = dot(jnp.concatenate([high, low], axis=0), mz[0])
        count = high.shape[0]
        result = most[:count] + most[count:] + dot(high, mz[1])
        for n, i in enumerate(batch):
            q, g = chunks[i]
            factor = inverse[q * xc:(q + 1) * xc].reshape(height, -1)
            for k in range(pack):
                at_line = (n * pack + k) * height
                held[i, k] = result[at_line:at_line + height] * factor
            stores.append(pltpu.make_async_copy(
                held.at[i], out.at[pl.ds(g * pack, pack), pl.ds(q * height, height)], store_sem.at[i]
            ))
            stores[-1].start()

    sent = send_a.at[:, :, pl.ds(0, rows - 1)]
    pltpu.make_async_copy(sent, sent, a_send).wait()
    sent = send_b.at[:, :, pl.ds(0, cols - 1)]
    pltpu.make_async_copy(sent, sent, b_send).wait()
    for store in stores:
        store.wait()


def on_device(rows, cols, species, symbol_x, symbol_y, symbol_z):
    fields, x, yl, zl = species.shape
    y, z = symbol_y.shape[0], symbol_z.shape[0]
    xb, yb = x // rows, y // cols
    pack = LANES // zl
    groups = fields // pack
    cuts = 2
    xc = xb // cuts

    hx = table(x)
    eye = np.eye(yl, dtype=np.float32)
    full_x = np.einsum("rqia,yb->qriyab", hx.T.reshape(rows, cuts, xc, x), eye).reshape(cuts, rows * xc * yl, x * yl)
    hy = table(y).T.reshape(cols, yb, rows, yl)
    full_y = np.einsum("cmry,ij->cimrjy", hy, np.eye(xc, dtype=np.float32)).reshape(cols * xc * yb, rows * xc * yl)
    tables = [
        np.concatenate(list(halves(full_x)), axis=1), np.concatenate(list(halves(full_y)), axis=0), halves(table(z))
    ]

    any_space = pl.BlockSpec(memory_space=pltpu.MemorySpace.HBM)
    chunks = cuts * groups
    a_shape = (cuts, groups, rows, xc * yl, LANES)
    b_shape = (cuts, groups, cols, xc * yb, LANES)
    dma = pltpu.SemaphoreType.DMA
    out = pl.pallas_call(
        functools.partial(kernel, (fields, pack, rows, cols, cuts, xc, yb, zl)),
        out_shape=pltpu.MemorySpace.VMEM((fields, xb * yb, z), jnp.float32),
        in_specs=[any_space] * 7,
        out_specs=pl.BlockSpec(memory_space=pl.ANY),
        scratch_shapes=[
            pltpu.VMEM((fields, x * yl, zl), jnp.float32),
            pltpu.VMEM(tables[0].shape, jnp.bfloat16),
            pltpu.VMEM(tables[1].shape, jnp.bfloat16),
            pltpu.VMEM(tables[2].shape, jnp.bfloat16),
            pltpu.SMEM((x,), jnp.float32),
            pltpu.SMEM((y,), jnp.float32),
            pltpu.VMEM((1, z), jnp.float32),
            pltpu.VMEM(a_shape, jnp.float32),
            pltpu.VMEM(a_shape, jnp.float32),
            pltpu.VMEM(b_shape, jnp.float32),
            pltpu.VMEM(b_shape, jnp.float32),
            pltpu.VMEM((xb, yb, z), jnp.float32),
            pltpu.VMEM((chunks, pack, xc * yb, z), jnp.float32),
            dma((fields + cuts + 5,)),
            dma((chunks,)),
            dma,
            dma((chunks,)),
            dma,
            dma((chunks,)),
        ],
        compiler_params=pltpu.CompilerParams(
            collective_id=0, has_side_effects=True, vmem_limit_bytes=60 * 1024 * 1024
        ),
    )(
        species.reshape(fields, x * yl, zl), symbol_x, symbol_y, symbol_z.reshape(1, z),
        *[jnp.asarray(t) for t in tables],
    )
    return out.reshape(fields, xb, yb, z)


def solution(mesh):
    placed = (P(None, None, "row", "col"), P(), P(), P())
    return jax.shard_map(
        functools.partial(on_device, mesh.shape["row"], mesh.shape["col"]),
        mesh=mesh,
        in_specs=placed,
        out_specs=P(None, "row", "col", None),
        check_vma=False,
    )
```
